32 devices in a mesh: grp: 2 (over x), scen: 16 (over z, y, core).
Axes of the slice: x: 2, y: 2, z: 4, core: 2. Of those that a mesh axis runs over, the one named last changes fastest.
Arguments:
- shocks: bfloat16 [32768, 2048], P(('grp', 'scen')), parts along dimension 0, may hold values from -8 to 8
- factor_sens: bfloat16 [2048, 1024], replicated, may hold values from -0.13258252 to 0.13258252
- notional: float32 [1024], replicated, may hold values from -0.25 to 0.25
- moneyness: float32 [1024], replicated, may hold values from -2 to 2
- desk_entity: int32 [64], replicated, may hold values from 0 to 7
- scenario_counts: int32 [32], P(('grp', 'scen')), parts along dimension 0, may hold values from 256 to 1024, as said below
- candidate_ids: int32 [2048], P('grp'), parts along dimension 0, may hold values from 0 to 16383, as said below
Outputs:
- tail_losses: float32 [512], P('grp'), parts along dimension 0
- cand_entity: float32 [2048, 8], P(('grp', 'scen')), parts along dimension 0
The draws below stay inside these ranges and needn't reach their ends.
There are 2 independent parts, one for each index of `grp`. The reference program is written for one: setup_inputs(seed, part) draws one part's arguments, and reference() takes and returns one part's arrays. A program takes and returns all parts, laid end to end along the dimension named above; an argument that names none is the same for every part. Nothing has to cross between parts.
Inputs may be any that keep to these rules, and one draw needn't show every extreme that they name: `scenario_counts`: every block has at least 256 valid scenarios; some block in every draw is full. `candidate_ids`: each id b * 1024 + j names a valid scenario: j is below scenario_counts[b].
All inputs are finite; a program needn't handle non-finite values.
Results may differ from the reference program's by a relative error of at most 0.0003.
Values sent between devices are 32-bit elements; how exact they have to be, the bound alone decides.
A program may use at most 128 MiB of HBM per device.

```python
import jax
import jax.numpy as jnp
from jax import lax

F = 2048
K = 64
INSTR = 16
ENT = 8
TOPK = 256
CAND = 1024
S_DEV = 1024
N_SCEN = 16


def common_draw(key):
    base = jax.random.fold_in(key, 7)
    key_a, key_b, key_c, key_d = jax.random.split(base, 4)
    counts = jax.random.randint(key_a, (N_SCEN,), S_DEV // 4, S_DEV + 1)
    filled = jax.random.randint(key_b, (), 0, N_SCEN)
    counts = jnp.where(jnp.arange(N_SCEN) == filled, S_DEV, counts).astype(jnp.int32)
    owners = jax.random.randint(key_c, (CAND,), 0, N_SCEN)
    offsets = jax.random.randint(key_d, (CAND,), 0, counts[owners])
    return (counts, (owners * S_DEV + offsets).astype(jnp.int32), filled)


def draw_scenario_counts(key, part):
    return common_draw(key)[0]


def draw_candidate_ids(key, part):
    return common_draw(key)[1]


def draw_shocks(key, part):
    filled = common_draw(key)[2]
    noise_key = jax.random.fold_in(key, 11)
    moves = jax.random.normal(noise_key, (S_DEV * N_SCEN, F), jnp.float32)
    hot_scale = 2.0
    block_of_row = jnp.arange(S_DEV * N_SCEN, dtype=jnp.int32) // S_DEV
    scales = jnp.where(block_of_row == filled, jnp.float32(hot_scale), jnp.float32(1.0))
    return jnp.clip(moves * scales[:, None], -8.0, 8.0).astype(jnp.bfloat16)


def draw_factor_sens(key, part):
    half = K * INSTR // 2
    key_a, key_b = jax.random.split(jax.random.fold_in(key, 21))
    first = jnp.clip(jax.random.normal(key_a, (F, half), jnp.float32), -4.0, 4.0)
    second = jnp.clip(jax.random.normal(key_b, (F, half), jnp.float32), -4.0, 4.0)
    paired = jnp.stack([first, -first + 0.15 * second], axis=2).reshape(F, K * INSTR)
    return (paired * F ** (-0.5)).astype(jnp.bfloat16)


def draw_notional(key, part):
    half = K * INSTR // 2
    scale = 2.0 * (K * INSTR) ** (-0.5)
    noise_key = jax.random.fold_in(key, 31)
    values = jnp.clip(jax.random.normal(noise_key, (half,), jnp.float32), -4.0, 4.0)
    return jnp.repeat(values * scale, 2).astype(jnp.float32)


def draw_moneyness(key, part):
    half = K * INSTR // 2
    noise_key = jax.random.fold_in(key, 41)
    values = jax.random.uniform(noise_key, (half,), jnp.float32, -2.0, 2.0)
    return jnp.repeat(values, 2).astype(jnp.float32)


def set_ends(entries, stream_key, least, top_value):
    longest = entries.shape.index(max(entries.shape))
    spots = []
    for shift in (0, 1):
        where = [jax.random.randint(jax.random.fold_in(stream_key, axis), (), 0, length) for axis, length in enumerate(entries.shape)]
        where[longest] = (where[longest] + shift) % entries.shape[longest]
        spots.append(tuple(where))
    return entries.at[spots[0]].set(least).at[spots[1]].set(top_value)


def setup_inputs(seed: int = 0, part: int = 0) -> dict:
    arg_keys = jax.random.split(jax.random.key(seed), 8)
    part_keys = jax.random.split(jax.random.fold_in(arg_keys[7], part), 8)
    shocks = draw_shocks(jax.random.fold_in(jax.random.fold_in(arg_keys[7], part), 71), part)
    factor_sens = draw_factor_sens(jax.random.fold_in(arg_keys[7], 71), part)
    notional = draw_notional(jax.random.fold_in(arg_keys[7], 71), part)
    moneyness = draw_moneyness(jax.random.fold_in(arg_keys[7], 71), part)
    desk_entity = set_ends(jax.random.randint(arg_keys[4], (K,), 0, ENT), jax.random.fold_in(arg_keys[4], 1), 0, ENT - 1).astype(jnp.int32)
    scenario_counts = draw_scenario_counts(jax.random.fold_in(jax.random.fold_in(arg_keys[7], part), 71), part)
    candidate_ids = draw_candidate_ids(jax.random.fold_in(jax.random.fold_in(arg_keys[7], part), 71), part)
    return {"shocks": shocks, "factor_sens": factor_sens, "notional": notional, "moneyness": moneyness, "desk_entity": desk_entity, "scenario_counts": scenario_counts, "candidate_ids": candidate_ids}


def price(rows, factor_sens, notional, moneyness):
    value = jnp.dot(rows, factor_sens, preferred_element_type=jnp.float32)
    inst = notional * (jax.nn.softplus(value + moneyness) - jax.nn.softplus(moneyness))
    return jnp.sum(inst.reshape(rows.shape[0], K, INSTR), axis=2)


def reference(shocks, factor_sens, notional, moneyness, desk_entity, scenario_counts, candidate_ids):
    blocks = shocks.reshape(N_SCEN, S_DEV, F)

    def one_block(item):
        rows, count = item
        loss = -jnp.sum(price(rows, factor_sens, notional, moneyness), axis=1)
        valid = jnp.arange(S_DEV, dtype=jnp.int32) < count
        return jnp.where(valid, loss, jnp.float32(-1e30))

    losses = lax.map(one_block, (blocks, scenario_counts))
    tail_losses = lax.top_k(losses.reshape(-1), TOPK)[0]
    cand_rows = jnp.take(shocks, candidate_ids, axis=0)
    cand_pnl = price(cand_rows, factor_sens, notional, moneyness)
    onehot = (desk_entity[:, None] == jnp.arange(ENT, dtype=jnp.int32)[None, :]).astype(jnp.float32)
    cand_entity = -jnp.dot(cand_pnl, onehot, precision=lax.Precision.HIGHEST)
    return tail_losses, cand_entity
```

```python
import functools

import jax
import jax.numpy as jnp
from jax import lax
from jax.experimental import pallas as pl
from jax.experimental.pallas import tpu as pltpu
from jax.sharding import PartitionSpec as P

INSTR = 16
ENT = 8
TOPK = 256
LANES = 128
BLOCK = 128
LOW = -1e30


def bitonic_sort(x, ascending):
    lane = lax.broadcasted_iota(jnp.int32, (x.shape[0], LANES), 1)
    parts = [x[:, p * LANES : (p + 1) * LANES] for p in range(TOPK // LANES)]
    a, b = parts
    big, small = jnp.maximum(a, b), jnp.minimum(a, b)
    parts = [jnp.where(ascending, small, big), jnp.where(ascending, big, small)]
    step = LANES // 2
    while step:
        first = (lane & step) == 0
        keep_big = first != ascending
        out = []
        for p in parts:
            other = jnp.where(first, pltpu.roll(p, LANES - step, 1), pltpu.roll(p, step, 1))
            out.append(jnp.where(keep_big, jnp.maximum(p, other), jnp.minimum(p, other)))
        parts = out
        step //= 2
    return jnp.concatenate(parts, axis=1)


def kernel(
    n,
    chunk,
    ent_ref,
    count_ref,
    shocks_hbm,
    sens_hbm,
    notional_ref,
    money_ref,
    ids_ref,
    tail_ref,
    cand_ref,
    shocks,
    sens,
    value,
    weight,
    sums,
    row_loss,
    col_loss,
    tail_send,
    tail_recv,
    cand_send,
    cand_recv,
    merged,
    flipped,
    x_sem,
    w_sem,
    tail_ssem,
    tail_rsem,
    cand_ssem,
    cand_rsem,
):
    slots, factors = shocks.shape
    cols = sens.shape[1]
    turns = slots // BLOCK
    me = lax.axis_index("scen")

    wcopies = []
    for q in range(4):
        width = cols // 4
        c = pltpu.make_async_copy(
            sens_hbm.at[:, pl.ds(q * width, width)], sens.at[:, pl.ds(q * width, width)], w_sem.at[q]
        )
        c.start()
        wcopies.append(c)

    def rows_copy(i):
        return pltpu.make_async_copy(
            shocks_hbm.at[pl.ds(i * BLOCK, BLOCK), :], shocks.at[pl.ds(i * BLOCK, BLOCK), :], x_sem.at[i]
        )

    for i in range(turns):
        rows_copy(i).start()

    barrier = pltpu.get_barrier_semaphore()
    for k in range(1, n):
        pl.semaphore_signal(barrier, inc=1, device_id={"scen": lax.rem(me + k, n)}, device_id_type=pl.DeviceIdType.MESH)

    wlane = lax.broadcasted_iota(jnp.int32, (INSTR, 2 * LANES), 1)
    for k in range(cols // INSTR):
        hit = (wlane == ent_ref[k]) | (wlane >= LANES)
        weight[k * INSTR : (k + 1) * INSTR, :] = jnp.where(hit, -1.0, 0.0).astype(jnp.bfloat16)

    money = money_ref[...]
    notional = notional_ref[...]
    base = jnp.maximum(money, 0.0) + jnp.log(1.0 + jnp.exp(-jnp.abs(money)))

    def matmul(i, slot):
        x = shocks[pl.ds(pl.multiple_of(i * BLOCK, BLOCK), BLOCK), :]
        value[slot] = jnp.dot(x, sens[...], preferred_element_type=jnp.float32)

    def finish(i, slot):
        z = value[slot] + money
        inst = notional * (jnp.maximum(z, 0.0) + jnp.log(1.0 + jnp.exp(-jnp.abs(z))) - base)
        hi = inst.astype(jnp.bfloat16)
        lo = (inst - hi.astype(jnp.float32)).astype(jnp.bfloat16)
        w = weight[...]
        total = jnp.dot(hi, w, preferred_element_type=jnp.float32) + jnp.dot(lo, w, preferred_element_type=jnp.float32)
        sums[pl.ds(pl.multiple_of(i * BLOCK, BLOCK), BLOCK), :] = total

    for c in wcopies:
        c.wait()
    rows_copy(0).wait()
    matmul(0, 0)

    def step(i, unused):
        rows_copy(i).wait()
        matmul(i, lax.rem(i, 2))
        finish(i - 1, lax.rem(i - 1, 2))
        return unused

    lax.fori_loop(1, turns, step, 0)
    finish(turns - 1, (turns - 1) % 2)

    count = count_ref[0]
    sub = lax.broadcasted_iota(jnp.int32, (LANES, LANES), 0)
    for t in range(slots // LANES):
        loss = sums[t * LANES : (t + 1) * LANES, LANES:]
        loss = jnp.where(sub + t * LANES < count, loss, LOW)
        col_loss[t * LANES : (t + 1) * LANES, :] = loss
        row_loss[:, t * LANES : (t + 1) * LANES] = loss.T[:8, :]
    rank = lax.broadcasted_iota(jnp.int32, (LANES, LANES), 1)
    order = lax.select(me >= n // 2, 1, 0)
    rank_lo = (rank + order * (TOPK - 1 - 2 * rank)).astype(jnp.float32)
    rank_hi = (rank + LANES + order * (TOPK - 1 - 2 * (rank + LANES))).astype(jnp.float32)
    ones = jnp.ones((LANES, LANES), jnp.bfloat16)

    def ranked(t, best):
        mine = col_loss[pl.ds(pl.multiple_of(t * LANES, LANES), LANES), :]
        larger = jnp.zeros((LANES, LANES), jnp.float32)
        for s in range(slots // LANES):
            theirs = row_loss[0:1, s * LANES : (s + 1) * LANES]
            larger = larger + jnp.where(theirs > mine, 1.0, 0.0)
        place = jnp.dot(larger.astype(jnp.bfloat16), ones, preferred_element_type=jnp.float32)
        b_lo, b_hi = best
        b_lo = jnp.minimum(b_lo, jnp.min(jnp.where(place <= rank_lo, mine, jnp.inf), axis=0, keepdims=True))
        b_hi = jnp.minimum(b_hi, jnp.min(jnp.where(place <= rank_hi, mine, jnp.inf), axis=0, keepdims=True))
        return b_lo, b_hi

    empty = jnp.full((1, LANES), jnp.inf, jnp.float32)
    b_lo, b_hi = lax.fori_loop(0, slots // LANES, ranked, (empty, empty))
    top = jnp.concatenate([b_lo, b_hi], axis=1)
    tail_send[...] = top
    tail_recv[me] = top

    pl.semaphore_wait(barrier, n - 1)

    def tail_copy(k):
        return pltpu.make_async_remote_copy(
            src_ref=tail_send,
            dst_ref=tail_recv.at[me],
            send_sem=tail_ssem.at[k],
            recv_sem=tail_rsem.at[k],
            device_id={"scen": lax.rem(me + k, n)},
            device_id_type=pl.DeviceIdType.MESH,
        )

    def cand_copy(k):
        peer = lax.rem(me + k, n)
        return pltpu.make_async_remote_copy(
            src_ref=cand_send.at[lax.div(peer * chunk, LANES)],
            dst_ref=cand_recv.at[me],
            send_sem=cand_ssem.at[k],
            recv_sem=cand_rsem.at[k],
            device_id={"scen": peer},
            device_id_type=pl.DeviceIdType.MESH,
        )

    for k in range(1, n):
        tail_copy(k).start()

    entity = jnp.concatenate(
        [sums[t * LANES : (t + 1) * LANES, :LANES].T[:ENT, :] for t in range(slots // LANES)], axis=1
    )
    hi = entity.astype(jnp.bfloat16)
    rest = entity - hi.astype(jnp.float32)
    mid = rest.astype(jnp.bfloat16)
    lo = (rest - mid.astype(jnp.float32)).astype(jnp.bfloat16)
    split = jnp.concatenate([hi.astype(jnp.float32), mid.astype(jnp.float32), lo.astype(jnp.float32)], axis=0)
    split = split.astype(jnp.bfloat16)
    width = 2 * LANES
    for q in range(ids_ref.shape[1] // width):
        local = ids_ref[:, q * width : (q + 1) * width] - me * slots
        hot = lax.broadcasted_iota(jnp.int32, (slots, width), 0) == local
        hot = jnp.where(hot, 1.0, 0.0).astype(jnp.bfloat16)
        got = jnp.dot(split, hot, preferred_element_type=jnp.float32)
        got = got[:ENT] + got[ENT : 2 * ENT] + got[2 * ENT :]
        for h in range(width // LANES):
            cand_send[q * (width // LANES) + h] = got[:, h * LANES : (h + 1) * LANES]
    mine_block = lax.div(me * chunk, LANES)
    cand_recv[me] = cand_send[mine_block]
    for k in range(1, n):
        cand_copy(k).start()

    for k in range(1, n):
        tail_copy(k).wait_recv()
    for b in range(n):
        merged[b : b + 1, :] = tail_recv[b]
    lists = n
    while lists > 1:
        half = lists // 2
        if lists == n:
            x = merged[...]
        x = jnp.maximum(x[:half], x[half : 2 * half])
        pad = max(half, 8)
        if half < 8:
            x = jnp.concatenate([x] * (pad // half), axis=0)
        row = lax.broadcasted_iota(jnp.int32, (pad, LANES), 0)
        ascending = row >= (half // 2 if half > 1 else pad)
        x = bitonic_sort(x, ascending)
        lists = half
    tail_ref[...] = x[:1, :]

    for k in range(1, n):
        cand_copy(k).wait_recv()
    total = cand_recv[0]
    for b in range(1, n):
        total = total + cand_recv[b]
    square = jnp.concatenate([total, jnp.zeros((LANES - ENT, LANES), jnp.float32)], axis=0)
    flipped[...] = square.T
    offset = lax.rem(me * chunk, LANES)
    cand_ref[...] = flipped[pl.ds(pl.multiple_of(offset, 8), chunk), :ENT]
    for k in range(1, n):
        tail_copy(k).wait_send()
        cand_copy(k).wait_send()


def body(n, shocks, factor_sens, notional, moneyness, desk_entity, scenario_counts, candidate_ids):
    slots, factors = shocks.shape
    cols = factor_sens.shape[1]
    cands = candidate_ids.shape[0]
    chunk = cands // n
    vmem = pl.BlockSpec(memory_space=pltpu.VMEM)
    smem = pl.BlockSpec(memory_space=pltpu.SMEM)
    hbm = pl.BlockSpec(memory_space=pl.ANY)
    tail, cand = pl.pallas_call(
        functools.partial(kernel, n, chunk),
        out_shape=(
            jax.ShapeDtypeStruct((1, TOPK), jnp.float32),
            jax.ShapeDtypeStruct((chunk, ENT), jnp.float32),
        ),
        in_specs=[smem, smem, hbm, hbm, vmem, vmem, vmem],
        out_specs=(vmem, vmem),
        scratch_shapes=[
            pltpu.VMEM((slots, factors), jnp.bfloat16),
            pltpu.VMEM((factors, cols), jnp.bfloat16),
            pltpu.VMEM((2, BLOCK, cols), jnp.float32),
            pltpu.VMEM((cols, 2 * LANES), jnp.bfloat16),
            pltpu.VMEM((slots, 2 * LANES), jnp.float32),
            pltpu.VMEM((8, slots), jnp.float32),
            pltpu.VMEM((slots, LANES), jnp.float32),
            pltpu.VMEM((1, TOPK), jnp.float32),
            pltpu.VMEM((n, 1, TOPK), jnp.float32),
            pltpu.VMEM((cands // LANES, ENT, LANES), jnp.float32),
            pltpu.VMEM((n, ENT, LANES), jnp.float32),
            pltpu.VMEM((n, TOPK), jnp.float32),
            pltpu.VMEM((LANES, LANES), jnp.float32),
            pltpu.SemaphoreType.DMA((slots // BLOCK,)),
            pltpu.SemaphoreType.DMA((4,)),
            pltpu.SemaphoreType.DMA((n,)),
            pltpu.SemaphoreType.DMA((n,)),
            pltpu.SemaphoreType.DMA((n,)),
            pltpu.SemaphoreType.DMA((n,)),
        ],
        compiler_params=pltpu.CompilerParams(
            collective_id=0, has_side_effects=True, vmem_limit_bytes=48 * 1024 * 1024
        ),
    )(
        desk_entity,
        scenario_counts,
        shocks,
        factor_sens,
        notional.reshape(1, cols),
        moneyness.reshape(1, cols),
        candidate_ids.reshape(1, cands),
    )
    return tail.reshape(TOPK), cand


def solution(mesh):
    return jax.shard_map(
        functools.partial(body, mesh.shape["scen"]),
        mesh=mesh,
        in_specs=(P(("grp", "scen"), None), P(), P(), P(), P(), P(("grp", "scen")), P("grp")),
        out_specs=(P("grp"), P(("grp", "scen"), None)),
        check_vma=False,
    )
```

```python
import functools

import jax
import jax.numpy as jnp
from jax import lax
from jax.experimental import pallas as pl
from jax.experimental.pallas import tpu as pltpu
from jax.sharding import PartitionSpec as P

INSTR = 16
ENT = 8
TOPK = 256
LANES = 128
LOW = -1e30


def bitonic_sort(x, ascending):
    lane = lax.broadcasted_iota(jnp.int32, (x.shape[0], LANES), 1)
    parts = [x[:, p * LANES : (p + 1) * LANES] for p in range(TOPK // LANES)]
    a, b = parts
    big, small = jnp.maximum(a, b), jnp.minimum(a, b)
    parts = [jnp.where(ascending, small, big), jnp.where(ascending, big, small)]
    step = LANES // 2
    while step:
        first = (lane & step) == 0
        keep_big = first != ascending
        out = []
        for p in parts:
            other = jnp.where(first, pltpu.roll(p, LANES - step, 1), pltpu.roll(p, step, 1))
            out.append(jnp.where(keep_big, jnp.maximum(p, other), jnp.minimum(p, other)))
        parts = out
        step //= 2
    return jnp.concatenate(parts, axis=1)


def kernel(
    n,
    chunk,
    count_ref,
    ent_hbm,
    shocks_hbm,
    sens_hbm,
    notional_hbm,
    money_hbm,
    ids_hbm,
    tail_ref,
    cand_ref,
    ent_ref,
    notional_ref,
    money_ref,
    ids_ref,
    base_ref,
    shocks,
    sens,
    value_a,
    value_b,
    weight,
    sums,
    row_loss,
    col_loss,
    tail_send,
    tail_recv,
    cand_send,
    cand_recv,
    merged,
    x_sem,
    w_sem,
    small_sem,
    tail_ssem,
    tail_rsem,
    cand_ssem,
    cand_rsem,
):
    slots, factors = shocks.shape
    quarters, _, width = sens.shape
    cols = quarters * width
    rows = value_a.shape[0]
    steps = (slots // rows) * quarters
    me = lax.axis_index("scen")

    def w_copy(q):
        return pltpu.make_async_copy(sens_hbm.at[:, pl.ds(q * width, width)], sens.at[q], w_sem.at[q])

    def x_copy(h):
        return pltpu.make_async_copy(
            shocks_hbm.at[pl.ds(h * rows, rows), :], shocks.at[pl.ds(h * rows, rows), :], x_sem.at[h]
        )

    small = [pltpu.make_async_copy(ent_hbm, ent_ref, small_sem.at[0])]
    for q in range(quarters):
        part = pl.ds(q * width, width)
        small.append(pltpu.make_async_copy(notional_hbm.at[:, part], notional_ref.at[q], small_sem.at[1 + 2 * q]))
        small.append(pltpu.make_async_copy(money_hbm.at[:, part], money_ref.at[q], small_sem.at[2 + 2 * q]))
    ids_copy = pltpu.make_async_copy(ids_hbm, ids_ref, small_sem.at[1 + 2 * quarters])
    for c in small:
        c.start()
    w_copy(0).start()
    x_copy(0).start()
    for q in range(1, quarters):
        w_copy(q).start()
    for h in range(1, slots // rows):
        x_copy(h).start()
    ids_copy.start()

    barrier = pltpu.get_barrier_semaphore()
    for k in range(1, n):
        pl.semaphore_signal(barrier, inc=1, device_id={"scen": lax.rem(me + k, n)}, device_id_type=pl.DeviceIdType.MESH)

    for c in small:
        c.wait()
    wlane = lax.broadcasted_iota(jnp.int32, (INSTR, 2 * LANES), 1)
    for k in range(cols // INSTR):
        hit = (wlane == ent_ref[k]) | (wlane >= LANES)
        weight[k * INSTR : (k + 1) * INSTR, :] = jnp.where(hit, -1.0, 0.0).astype(jnp.bfloat16)
    money = money_ref[...]
    base_ref[...] = jnp.maximum(money, 0.0) + jnp.log(1.0 + jnp.exp(-jnp.abs(money)))
    sums[...] = jnp.zeros_like(sums)

    def matmul(s, value):
        h, q = lax.div(s, quarters), lax.rem(s, quarters)
        x = shocks[pl.ds(pl.multiple_of(h * rows, rows), rows), :]
        value[...] = jnp.dot(x, sens[q], preferred_element_type=jnp.float32)

    def finish(s, value):
        h, q = lax.div(s, quarters), lax.rem(s, quarters)
        z = value[...] + money_ref[q]
        inst = notional_ref[q] * (jnp.maximum(z, 0.0) + jnp.log(1.0 + jnp.exp(-jnp.abs(z))) - base_ref[q])
        hi = inst.astype(jnp.bfloat16)
        lo = (inst - hi.astype(jnp.float32)).astype(jnp.bfloat16)
        w = weight[pl.ds(pl.multiple_of(q * width, width), width), :]
        total = jnp.dot(hi, w, preferred_element_type=jnp.float32) + jnp.dot(lo, w, preferred_element_type=jnp.float32)
        sums[pl.ds(pl.multiple_of(h * rows, rows), rows), :] += total

    def arrive(s):
        for q in range(1, quarters):
            @pl.when(s == q)
            def _():
                w_copy(q).wait()
        for h in range(1, slots // rows):
            @pl.when(s == h * quarters)
            def _():
                x_copy(h).wait()

    w_copy(0).wait()
    x_copy(0).wait()
    matmul(0, value_a)

    def pair(j, unused):
        arrive(2 * j + 1)
        arrive(2 * j + 2)
        matmul(2 * j + 1, value_b)
        finish(2 * j, value_a)
        matmul(2 * j + 2, value_a)
        finish(2 * j + 1, value_b)
        return unused

    lax.fori_loop(0, steps // 2 - 1, pair, 0)
    arrive(jnp.int32(steps - 1))
    matmul(steps - 1, value_b)
    finish(steps - 2, value_a)
    finish(steps - 1, value_b)

    def cand_copy(k):
        peer = lax.rem(me + k, n)
        return pltpu.make_async_remote_copy(
            src_ref=cand_send.at[peer],
            dst_ref=cand_recv.at[me],
            send_sem=cand_ssem.at[k],
            recv_sem=cand_rsem.at[k],
            device_id={"scen": peer},
            device_id_type=pl.DeviceIdType.MESH,
        )

    entity = jnp.concatenate(
        [sums[t * LANES : (t + 1) * LANES, :LANES].T[:ENT, :] for t in range(slots // LANES)], axis=1
    )
    hi = entity.astype(jnp.bfloat16).astype(jnp.float32)
    rest = entity - hi
    mid = rest.astype(jnp.bfloat16).astype(jnp.float32)
    split = jnp.concatenate([hi, mid, rest - mid], axis=0).astype(jnp.bfloat16)
    ids_copy.wait()
    packed = cand_send.shape[1]
    lane = lax.broadcasted_iota(jnp.int32, (packed, LANES), 1)
    span = 2 * LANES
    for p in range(ids_ref.shape[1] // span):
        local = ids_ref[:, p * span : (p + 1) * span] - me * slots
        hot = lax.broadcasted_iota(jnp.int32, (slots, span), 0) == local
        hot = jnp.where(hot, 1.0, 0.0).astype(jnp.bfloat16)
        got = jnp.dot(split, hot, preferred_element_type=jnp.float32)
        got = got[:ENT] + got[ENT : 2 * ENT] + got[2 * ENT :]
        for d in range(span // chunk):
            first = d * chunk // LANES * LANES
            offset = d * chunk - first
            message = None
            for j in range(ENT // packed):
                piece = got[j * packed : (j + 1) * packed, first : first + LANES]
                shift = (j * chunk - offset) % LANES
                if shift:
                    piece = pltpu.roll(piece, shift, 1)
                message = piece if message is None else jnp.where(lane >= j * chunk, piece, message)
            cand_send[p * (span // chunk) + d] = message
    cand_recv[me] = cand_send[me]

    pl.semaphore_wait(barrier, n - 1)
    for k in range(1, n):
        cand_copy(k).start()

    count = count_ref[0]
    sub = lax.broadcasted_iota(jnp.int32, (LANES, LANES), 0)
    for t in range(slots // LANES):
        loss = sums[t * LANES : (t + 1) * LANES, LANES:]
        loss = jnp.where(sub + t * LANES < count, loss, LOW)
        col_loss[t * LANES : (t + 1) * LANES, :] = loss
        row_loss[:, t * LANES : (t + 1) * LANES] = loss.T[:8, :]
    rank = lax.broadcasted_iota(jnp.int32, (LANES, LANES), 1)
    order = lax.select(me >= n // 2, 1, 0)
    rank_lo = (rank + order * (TOPK - 1 - 2 * rank)).astype(jnp.float32)
    rank_hi = (rank + LANES + order * (TOPK - 1 - 2 * (rank + LANES))).astype(jnp.float32)
    ones = jnp.ones((LANES, LANES), jnp.bfloat16)

    def ranked(t, best):
        mine = col_loss[pl.ds(pl.multiple_of(t * LANES, LANES), LANES), :]
        larger = jnp.zeros((LANES, LANES), jnp.float32)
        for s in range(slots // LANES):
            theirs = row_loss[0:1, s * LANES : (s + 1) * LANES]
            larger = larger + jnp.where(theirs > mine, 1.0, 0.0)
        place = jnp.dot(larger.astype(jnp.bfloat16), ones, preferred_element_type=jnp.float32)
        b_lo, b_hi = best
        b_lo = jnp.minimum(b_lo, jnp.min(jnp.where(place <= rank_lo, mine, jnp.inf), axis=0, keepdims=True))
        b_hi = jnp.minimum(b_hi, jnp.min(jnp.where(place <= rank_hi, mine, jnp.inf), axis=0, keepdims=True))
        return b_lo, b_hi

    empty = jnp.full((1, LANES), jnp.inf, jnp.float32)
    b_lo, b_hi = lax.fori_loop(0, slots // LANES, ranked, (empty, empty))
    top = jnp.concatenate([b_lo, b_hi], axis=1)
    tail_send[...] = top
    tail_recv[me] = top

    def tail_copy(k):
        return pltpu.make_async_remote_copy(
            src_ref=tail_send,
            dst_ref=tail_recv.at[me],
            send_sem=tail_ssem.at[k],
            recv_sem=tail_rsem.at[k],
            device_id={"scen": lax.rem(me + k, n)},
            device_id_type=pl.DeviceIdType.MESH,
        )

    for k in range(1, n):
        tail_copy(k).start()

    for k in range(1, n):
        tail_copy(k).wait_recv()
    for b in range(n):
        merged[b : b + 1, :] = tail_recv[b]
    lists = n
    while lists > 1:
        half = lists // 2
        if lists == n:
            x = merged[...]
        x = jnp.maximum(x[:half], x[half : 2 * half])
        pad = max(half, 8)
        if half < 8:
            x = jnp.concatenate([x] * (pad // half), axis=0)
        row = lax.broadcasted_iota(jnp.int32, (pad, LANES), 0)
        ascending = row >= (half // 2 if half > 1 else pad)
        x = bitonic_sort(x, ascending)
        lists = half
    tail_ref[...] = x[:1, :]

    for k in range(1, n):
        cand_copy(k).wait_recv()
    total = cand_recv[0]
    for b in range(1, n):
        total = total + cand_recv[b]
    cand_ref[...] = jnp.concatenate([total[:, j * chunk : (j + 1) * chunk] for j in range(ENT // packed)], axis=0)
    for k in range(1, n):
        tail_copy(k).wait_send()
        cand_copy(k).wait_send()


def deliver(tail_in, cand_in, tail_out, cand_out):
    tail_out[...] = tail_in[...]
    cand_out[...] = cand_in[...]


def body(n, shocks, factor_sens, notional, moneyness, desk_entity, scenario_counts, candidate_ids):
    slots, factors = shocks.shape
    cols = factor_sens.shape[1]
    cands = candidate_ids.shape[0]
    chunk = cands // n
    packed = ENT // min(ENT, LANES // chunk)
    width = cols // 4
    rows = slots // 2
    vmem = pl.BlockSpec(memory_space=pltpu.VMEM)
    smem = pl.BlockSpec(memory_space=pltpu.SMEM)
    hbm = pl.BlockSpec(memory_space=pltpu.HBM)
    shapes = (
        jax.ShapeDtypeStruct((1, TOPK), jnp.float32),
        jax.ShapeDtypeStruct((ENT, chunk), jnp.float32),
    )
    tail, cand = pl.pallas_call(
        functools.partial(kernel, n, chunk),
        out_shape=shapes,
        in_specs=[smem, hbm, hbm, hbm, hbm, hbm, hbm],
        out_specs=(vmem, vmem),
        scratch_shapes=[
            pltpu.SMEM(desk_entity.shape, jnp.int32),
            pltpu.VMEM((4, 1, width), jnp.float32),
            pltpu.VMEM((4, 1, width), jnp.float32),
            pltpu.VMEM((1, cands), jnp.int32),
            pltpu.VMEM((4, 1, width), jnp.float32),
            pltpu.VMEM((slots, factors), jnp.bfloat16),
            pltpu.VMEM((4, factors, width), jnp.bfloat16),
            pltpu.VMEM((rows, width), jnp.float32),
            pltpu.VMEM((rows, width), jnp.float32),
            pltpu.VMEM((cols, 2 * LANES), jnp.bfloat16),
            pltpu.VMEM((slots, 2 * LANES), jnp.float32),
            pltpu.VMEM((8, slots), jnp.float32),
            pltpu.VMEM((slots, LANES), jnp.float32),
            pltpu.VMEM((1, TOPK), jnp.float32),
            pltpu.VMEM((n, 1, TOPK), jnp.float32),
            pltpu.VMEM((n, packed, LANES), jnp.float32),
            pltpu.VMEM((n, packed, LANES), jnp.float32),
            pltpu.VMEM((n, TOPK), jnp.float32),
            pltpu.SemaphoreType.DMA((2,)),
            pltpu.SemaphoreType.DMA((4,)),
            pltpu.SemaphoreType.DMA((10,)),
            pltpu.SemaphoreType.DMA((n,)),
            pltpu.SemaphoreType.DMA((n,)),
            pltpu.SemaphoreType.DMA((n,)),
            pltpu.SemaphoreType.DMA((n,)),
        ],
        compiler_params=pltpu.CompilerParams(
            collective_id=0, has_side_effects=True, vmem_limit_bytes=67043328
        ),
    )(
        scenario_counts,
        desk_entity,
        shocks,
        factor_sens,
        notional.reshape(1, cols),
        moneyness.reshape(1, cols),
        candidate_ids.reshape(1, cands),
    )
    tail, cand = pl.pallas_call(deliver, out_shape=shapes, in_specs=[vmem, vmem], out_specs=(vmem, vmem))(tail, cand)
    return tail.reshape(TOPK), cand.T


def solution(mesh):
    return jax.shard_map(
        functools.partial(body, mesh.shape["scen"]),
        mesh=mesh,
        in_specs=(P(("grp", "scen"), None), P(), P(), P(), P(), P(("grp", "scen")), P("grp")),
        out_specs=(P("grp"), P(("grp", "scen"), None)),
        check_vma=False,
    )
```

```python
import functools

import jax
import jax.numpy as jnp
from jax import lax
from jax.experimental import pallas as pl
from jax.experimental.pallas import tpu as pltpu
from jax.sharding import PartitionSpec as P

INSTR = 16
ENT = 8
TOPK = 256
LANES = 128
LOW = -1e30


def bitonic_sort(x, ascending):
    lane = lax.broadcasted_iota(jnp.int32, (x.shape[0], LANES), 1)
    parts = [x[:, p * LANES : (p + 1) * LANES] for p in range(TOPK // LANES)]
    a, b = parts
    big, small = jnp.maximum(a, b), jnp.minimum(a, b)
    parts = [jnp.where(ascending, small, big), jnp.where(ascending, big, small)]
    step = LANES // 2
    while step:
        first = (lane & step) == 0
        keep_big = first != ascending
        out = []
        for p in parts:
            other = jnp.where(first, pltpu.roll(p, LANES - step, 1), pltpu.roll(p, step, 1))
            out.append(jnp.where(keep_big, jnp.maximum(p, other), jnp.minimum(p, other)))
        parts = out
        step //= 2
    return jnp.concatenate(parts, axis=1)


def kernel(
    n,
    chunk,
    count_ref,
    ent_hbm,
    shocks_hbm,
    sens_hbm,
    notional_hbm,
    money_hbm,
    ids_hbm,
    tail_ref,
    cand_ref,
    ent_ref,
    notional_ref,
    money_ref,
    ids_ref,
    base_ref,
    shocks,
    sens,
    value,
    weight,
    sums,
    entity,
    row_loss,
    col_loss,
    send,
    recv,
    merged,
    x_sem,
    w_sem,
    small_sem,
    send_sem,
    recv_sem,
):
    slots, factors = shocks.shape
    quarters, _, width = sens.shape
    cols = quarters * width
    rows = value.shape[0]
    groups = slots // rows
    half = groups // 2 * quarters
    steps = groups * quarters
    packed = send.shape[1] - TOPK // LANES
    me = lax.axis_index("scen")

    def w_copy(q):
        return pltpu.make_async_copy(
            sens_hbm.at[:, pl.ds(pl.multiple_of(q * width, width), width)], sens.at[q], w_sem.at[q]
        )

    def x_copy(h):
        part = pl.ds(pl.multiple_of(h * (slots // 2), slots // 2), slots // 2)
        return pltpu.make_async_copy(shocks_hbm.at[part, :], shocks.at[part, :], x_sem.at[h])

    small = [pltpu.make_async_copy(ent_hbm, ent_ref, small_sem.at[0])]
    for q in range(quarters):
        part = pl.ds(q * width, width)
        small.append(pltpu.make_async_copy(notional_hbm.at[:, part], notional_ref.at[q], small_sem.at[1 + 2 * q]))
        small.append(pltpu.make_async_copy(money_hbm.at[:, part], money_ref.at[q], small_sem.at[2 + 2 * q]))
    w_copy(0).start()
    x_copy(0).start()
    for c in small:
        c.start()
    for q in range(1, quarters):
        w_copy(q).start()
    x_copy(1).start()
    spans = ids_ref.shape[0]
    span = ids_ref.shape[2]
    ids_copies = [
        pltpu.make_async_copy(ids_hbm.at[:, pl.ds(p * span, span)], ids_ref.at[p], small_sem.at[1 + 2 * quarters + p])
        for p in range(spans)
    ]
    for c in ids_copies:
        c.start()

    barrier = pltpu.get_barrier_semaphore()

    def greet(k, unused):
        pl.semaphore_signal(
            barrier, inc=1, device_id={"scen": lax.rem(me + k, n)}, device_id_type=pl.DeviceIdType.MESH
        )
        return unused

    lax.fori_loop(1, n, greet, 0)

    for c in small:
        c.wait()
    wlane = lax.broadcasted_iota(jnp.int32, (INSTR, 2 * LANES), 1)

    def spread(k, unused):
        hit = (wlane == ent_ref[k]) | (wlane >= LANES)
        part = pl.ds(pl.multiple_of(k * INSTR, INSTR), INSTR)
        weight[part, :] = jnp.where(hit, -1.0, 0.0).astype(jnp.bfloat16)
        return unused

    lax.fori_loop(0, cols // INSTR, spread, 0)
    money = money_ref[...]
    base_ref[...] = jnp.maximum(money, 0.0) + jnp.log(1.0 + jnp.exp(-jnp.abs(money)))
    notional_ref[quarters] = jnp.zeros((1, width), jnp.float32)

    def clear(t, unused):
        part = pl.ds(pl.multiple_of(t * LANES, LANES), LANES)
        sums[part, :] = jnp.zeros((LANES, 2 * LANES), jnp.float32)
        return unused

    lax.fori_loop(0, slots // LANES, clear, 0)

    def clear_value(t, unused):
        part = pl.ds(pl.multiple_of(t * 64, 64), 64)
        value[part, :] = jnp.zeros((64, width), jnp.float32)
        return unused

    lax.fori_loop(0, rows // 64, clear_value, 0)

    def place(s):
        h = lax.div(s, half)
        q = lax.div(lax.rem(s, half), groups // 2)
        g = lax.rem(s, groups // 2)
        return q, pl.ds(pl.multiple_of((h * (groups // 2) + g) * rows, rows), rows)

    def step(s, unused):
        for q in range(quarters):
            @pl.when(s == q * (groups // 2))
            def _():
                w_copy(q).wait()
                if q == 0:
                    x_copy(0).wait()

        @pl.when(s == half)
        def _():
            x_copy(1).wait()

        q, part = place(lax.rem(s + steps - 1, steps))
        z = value[...] + money_ref[q]
        scale = notional_ref[lax.select(s == 0, quarters, q)]
        inst = scale * (jnp.maximum(z, 0.0) + jnp.log(1.0 + jnp.exp(-jnp.abs(z))) - base_ref[q])
        hi = inst.astype(jnp.bfloat16)
        lo = (inst - hi.astype(jnp.float32)).astype(jnp.bfloat16)
        w = weight[pl.ds(pl.multiple_of(q * width, width), width), :]
        total = jnp.dot(hi, w, preferred_element_type=jnp.float32) + jnp.dot(lo, w, preferred_element_type=jnp.float32)
        sums[part, :] += total
        q, part = place(lax.rem(s, steps))
        value[...] = jnp.dot(shocks[part, :], sens[q], preferred_element_type=jnp.float32)
        return unused

    lax.fori_loop(0, steps + 1, step, 0)

    count = count_ref[0]
    sub = lax.broadcasted_iota(jnp.int32, (LANES, LANES), 0)
    for c in ids_copies:
        c.wait()

    def arrange(t, unused):
        part = pl.ds(pl.multiple_of(t * LANES, LANES), LANES)
        loss = jnp.where(sub + t * LANES < count, sums[part, LANES:], LOW)
        col_loss[part, :] = loss
        row_loss[t] = loss.T[:8, :]
        sides = sums[part, :LANES].T[:ENT, :]
        hi = sides.astype(jnp.bfloat16).astype(jnp.float32)
        rest = sides - hi
        mid = rest.astype(jnp.bfloat16).astype(jnp.float32)
        entity[t] = jnp.concatenate([hi, mid, rest - mid, jnp.zeros_like(hi)], axis=0).astype(jnp.bfloat16)
        return unused

    lax.fori_loop(0, slots // LANES, arrange, 0)
    split = jnp.concatenate([entity[t] for t in range(slots // LANES)], axis=1)
    lane = lax.broadcasted_iota(jnp.int32, (packed, LANES), 1)

    def select(p, unused):
        local = ids_ref[p] - me * slots
        hot = lax.broadcasted_iota(jnp.int32, (slots, span), 0) == local
        hot = jnp.where(hot, 1.0, 0.0).astype(jnp.bfloat16)
        got = jnp.dot(split, hot, preferred_element_type=jnp.float32)
        got = got[:ENT] + got[ENT : 2 * ENT] + got[2 * ENT : 3 * ENT]
        for d in range(span // chunk):
            first = d * chunk // LANES * LANES
            offset = d * chunk - first
            message = None
            for j in range(ENT // packed):
                piece = got[j * packed : (j + 1) * packed, first : first + LANES]
                shift = (j * chunk - offset) % LANES
                if shift:
                    piece = pltpu.roll(piece, shift, 1)
                message = piece if message is None else jnp.where(lane >= j * chunk, piece, message)
            send[p * (span // chunk) + d, :packed, :] = message
        return unused

    lax.fori_loop(0, spans, select, 0)

    rank = lax.broadcasted_iota(jnp.int32, (LANES, LANES), 1)
    order = lax.select(me >= n // 2, 1, 0)
    rank_lo = (rank + order * (TOPK - 1 - 2 * rank)).astype(jnp.float32)
    rank_hi = (rank + LANES + order * (TOPK - 1 - 2 * (rank + LANES))).astype(jnp.float32)
    ones = jnp.ones((LANES, LANES), jnp.bfloat16)

    def ranked(t, best):
        mine = col_loss[pl.ds(pl.multiple_of(t * LANES, LANES), LANES), :]
        larger = jnp.zeros((LANES, LANES), jnp.float32)
        for s in range(slots // LANES):
            larger = larger + jnp.where(row_loss[s][:1, :] > mine, 1.0, 0.0)
        above = jnp.dot(larger.astype(jnp.bfloat16), ones, preferred_element_type=jnp.float32)
        b_lo, b_hi = best
        b_lo = jnp.minimum(b_lo, jnp.min(jnp.where(above <= rank_lo, mine, jnp.inf), axis=0, keepdims=True))
        b_hi = jnp.minimum(b_hi, jnp.min(jnp.where(above <= rank_hi, mine, jnp.inf), axis=0, keepdims=True))
        return b_lo, b_hi

    empty = jnp.full((1, LANES), jnp.inf, jnp.float32)
    b_lo, b_hi = lax.fori_loop(0, slots // LANES, ranked, (empty, empty))

    def attach(d, unused):
        send[d, packed : packed + 1, :] = b_lo
        send[d, packed + 1 :, :] = b_hi
        return unused

    lax.fori_loop(0, n, attach, 0)
    recv[me] = send[me]

    def message_copy(k):
        peer = lax.rem(me + k, n)
        return pltpu.make_async_remote_copy(
            src_ref=send.at[peer],
            dst_ref=recv.at[me],
            send_sem=send_sem.at[k],
            recv_sem=recv_sem.at[k],
            device_id={"scen": peer},
            device_id_type=pl.DeviceIdType.MESH,
        )

    pl.semaphore_wait(barrier, n - 1)

    def start(k, unused):
        message_copy(k).start()
        return unused

    def arrived(k, unused):
        message_copy(k).wait_recv()
        return unused

    def sent(k, unused):
        message_copy(k).wait_send()
        return unused

    lax.fori_loop(1, n, start, 0)
    lax.fori_loop(1, n, arrived, 0)

    total = jnp.zeros((packed, LANES), jnp.float32)
    for b in range(n):
        total = total + recv[b, :packed, :]
        merged[b : b + 1, :LANES] = recv[b, packed : packed + 1, :]
        merged[b : b + 1, LANES:] = recv[b, packed + 1 :, :]
    cand_ref[...] = jnp.concatenate([total[:, j * chunk : (j + 1) * chunk] for j in range(ENT // packed)], axis=0)
    x = merged[...]
    lists = n
    while lists > 1:
        keep = lists // 2
        x = jnp.maximum(x[:keep], x[keep : 2 * keep])
        pad = max(keep, 8)
        if keep < 8:
            x = jnp.concatenate([x] * (pad // keep), axis=0)
        row = lax.broadcasted_iota(jnp.int32, (pad, LANES), 0)
        x = bitonic_sort(x, row >= (keep // 2 if keep > 1 else pad))
        lists = keep
    tail_ref[...] = x[:1, :]
    lax.fori_loop(1, n, sent, 0)


def deliver(tail_in, cand_in, tail_out, cand_out):
    tail_out[...] = tail_in[...]
    cand_out[...] = cand_in[...]


def body(n, shocks, factor_sens, notional, moneyness, desk_entity, scenario_counts, candidate_ids):
    slots, factors = shocks.shape
    cols = factor_sens.shape[1]
    cands = candidate_ids.shape[0]
    chunk = cands // n
    packed = ENT // min(ENT, LANES // chunk)
    width = cols // 4
    rows = slots // 4
    span = 2 * LANES
    vmem = pl.BlockSpec(memory_space=pltpu.VMEM)
    smem = pl.BlockSpec(memory_space=pltpu.SMEM)
    hbm = pl.BlockSpec(memory_space=pltpu.HBM)
    shapes = (
        jax.ShapeDtypeStruct((1, TOPK), jnp.float32),
        jax.ShapeDtypeStruct((ENT, chunk), jnp.float32),
    )
    tail, cand = pl.pallas_call(
        functools.partial(kernel, n, chunk),
        out_shape=shapes,
        in_specs=[smem, hbm, hbm, hbm, hbm, hbm, hbm],
        out_specs=(vmem, vmem),
        scratch_shapes=[
            pltpu.SMEM(desk_entity.shape, jnp.int32),
            pltpu.VMEM((5, 1, width), jnp.float32),
            pltpu.VMEM((4, 1, width), jnp.float32),
            pltpu.VMEM((cands // span, 1, span), jnp.int32),
            pltpu.VMEM((4, 1, width), jnp.float32),
            pltpu.VMEM((slots, factors), jnp.bfloat16),
            pltpu.VMEM((4, factors, width), jnp.bfloat16),
            pltpu.VMEM((rows, width), jnp.float32),
            pltpu.VMEM((cols, 2 * LANES), jnp.bfloat16),
            pltpu.VMEM((slots, 2 * LANES), jnp.float32),
            pltpu.VMEM((slots // LANES, 4 * ENT, LANES), jnp.bfloat16),
            pltpu.VMEM((slots // LANES, 8, LANES), jnp.float32),
            pltpu.VMEM((slots, LANES), jnp.float32),
            pltpu.VMEM((n, packed + TOPK // LANES, LANES), jnp.float32),
            pltpu.VMEM((n, packed + TOPK // LANES, LANES), jnp.float32),
            pltpu.VMEM((n, TOPK), jnp.float32),
            pltpu.SemaphoreType.DMA((2,)),
            pltpu.SemaphoreType.DMA((4,)),
            pltpu.SemaphoreType.DMA((9 + cands // span,)),
            pltpu.SemaphoreType.DMA((n,)),
            pltpu.SemaphoreType.DMA((n,)),
        ],
        compiler_params=pltpu.CompilerParams(
            collective_id=0, has_side_effects=True, vmem_limit_bytes=67043328
        ),
    )(
        scenario_counts,
        desk_entity,
        shocks,
        factor_sens,
        notional.reshape(1, cols),
        moneyness.reshape(1, cols),
        candidate_ids.reshape(1, cands),
    )
    tail, cand = pl.pallas_call(deliver, out_shape=shapes, in_specs=[vmem, vmem], out_specs=(vmem, vmem))(tail, cand)
    return tail.reshape(TOPK), cand.T


def solution(mesh):
    return jax.shard_map(
        functools.partial(body, mesh.shape["scen"]),
        mesh=mesh,
        in_specs=(P(("grp", "scen"), None), P(), P(), P(), P(), P(("grp", "scen")), P("grp")),
        out_specs=(P("grp"), P(("grp", "scen"), None)),
        check_vma=False,
    )
```
